32 devices in a mesh: left: 8 (over z, x), right: 4 (over y, core).
Axes of the slice: x: 2, y: 2, z: 4, core: 2. Of those that a mesh axis runs over, the one named last changes fastest.
Arguments:
- species: float32 [4, 256, 128, 128], P(None, None, 'left', 'right'), may hold values from -6 to 6
- coupling: float32 [4, 4], replicated, may hold values from -4 to 4
- symbol_x: float32 [256], replicated, may hold values from 0.3 to 3
- symbol_y: float32 [128], replicated, may hold values from 0.3 to 3
- symbol_z: float32 [128], replicated, may hold values from 0.3 to 3
Outputs:
- modes: float32 [4, 256, 128, 128], P(None, 'left', 'right')
The draws below stay inside these ranges and needn't reach their ends.
All inputs are finite; a program needn't handle non-finite values.
Results may differ from the reference program's by a relative error of at most 0.000071.
Values sent between devices are 32-bit elements; how exact they have to be, the bound alone decides.
A program may use at most 128 MiB of HBM per device.

```python
import jax
import jax.numpy as jnp
from jax import lax

GRID_X = 256
GRID_Y = 128
GRID_Z = 128
FIELDS = 4


def block_scale(stream_key, dims, pieces, smallest, top_value):
    def one(position, blocks):
        draws = jax.random.uniform(jax.random.fold_in(jax.random.fold_in(stream_key, 6), position), (blocks,), jnp.float32, smallest / len(pieces), top_value / len(pieces))
        return jnp.repeat(jnp.exp(draws), dims[position] // blocks).reshape((-1,) + (1,) * (len(dims) - position - 1))

    level = one(*pieces[0])
    for cut in pieces[1:]:
        level = level * one(*cut)
    return level


def noise(own_key, dims, deviation, reach, cuts=(), dtype=jnp.bfloat16):
    gain = block_scale(own_key, dims, cuts, -0.22, 0.18) if cuts else 1.0
    array = jax.random.normal(own_key, dims, jnp.float32) * deviation * gain
    return jnp.minimum(jnp.maximum(array, -reach), reach).astype(dtype)


def setup_inputs(seed: int = 0) -> dict:
    streams_of = jax.random.split(jax.random.key(seed), 6)
    species = noise(streams_of[0], (FIELDS, GRID_X, GRID_Y, GRID_Z), 1.0, 6.0, ((2, 8), (3, 4)), jnp.float32)
    coupling = noise(streams_of[1], (FIELDS, FIELDS), 0.7, 4.0, (), jnp.float32)
    symbol_x = jnp.clip(jax.random.uniform(streams_of[2], (GRID_X,), jnp.float32, 0.3, 3.0), 0.3, 3.0)
    symbol_y = jnp.clip(jax.random.uniform(streams_of[3], (GRID_Y,), jnp.float32, 0.3, 3.0), 0.3, 3.0)
    symbol_z = jnp.clip(jax.random.uniform(streams_of[4], (GRID_Z,), jnp.float32, 0.3, 3.0), 0.3, 3.0)
    return {"species": species, "coupling": coupling, "symbol_x": symbol_x, "symbol_y": symbol_y, "symbol_z": symbol_z}


def basis_table(count):
    rank = jnp.arange(count)
    angle = (2.0 * jnp.pi / count) * ((rank[:, None] * rank[None, :]) % count).astype(jnp.float32)
    return (jnp.cos(angle) + jnp.sin(angle)) * (count ** -0.5)


def along_dim(values, dim):
    moved = jnp.tensordot(values, basis_table(values.shape[dim]), axes=([dim], [0]), precision=lax.Precision.HIGHEST)
    return jnp.moveaxis(moved, -1, dim)


def reference(species, coupling, symbol_x, symbol_y, symbol_z):
    modes = species
    modes = along_dim(modes, 1)
    modes = along_dim(modes, 2)
    modes = along_dim(modes, 3)
    symbol = symbol_x[:, None, None] + symbol_y[None, :, None] + symbol_z[None, None, :]
    weight_xyz = 1.0 / (1.0 + symbol)
    mixed_fields = jnp.einsum("ab,bxyz->axyz", coupling, modes, precision=lax.Precision.HIGHEST)
    modes = weight_xyz * modes + (1.0 - weight_xyz) * mixed_fields
    return modes
```

```python
import functools

import jax
import jax.numpy as jnp
import numpy as np
from jax import lax
from jax.experimental import pallas as pl
from jax.experimental.pallas import tpu as pltpu
from jax.sharding import PartitionSpec as P

MESH = pl.DeviceIdType.MESH
WINDOW = 12
PARTS = (6, 6, 6, 6, 4, 4)
GROUPS = 4


def chunk_sizes(block):
    unit = block // sum(PARTS)
    return [part * unit for part in PARTS] if unit and block % sum(PARTS) == 0 else [block]


def basis_table(count):
    rank = np.arange(count)
    angle = 2.0 * np.pi / count * (rank[:, None] * rank[None, :] % count)
    return (np.cos(angle) + np.sin(angle)) / np.sqrt(count)


def halves(table):
    table = table.astype(np.float32)
    high = table.astype(jnp.bfloat16)
    low = (table - high.astype(np.float32)).astype(jnp.bfloat16)
    return high, low


def split(values):
    high = values.astype(jnp.bfloat16)
    low = (values - high.astype(jnp.float32)).astype(jnp.bfloat16)
    return high, low


def kernel(
    n_left, n_right, sizes,
    x_hbm, hx_hbm, hy_hbm, wz_hbm, coup_hbm, sx_hbm, sy_hbm, sz_hbm,
    out_ref,
    x_buf, hx, hy, wz, coup_ref, sx_ref, sy_ref, sz_ref, send_a, recv_b, send_c, recv_d, z_buf, sy_cols,
    sem_x, sem_t, sem_as, sem_br, sem_cs, sem_dr,
):
    fields, share_y, share_z, size_x = x_hbm.shape
    size_y, size_z = sy_hbm.shape[1], sz_hbm.shape[1]
    lanes = fields * share_z
    block_x, block_y = size_x // n_left, size_y // n_right
    pairs = share_y // 2
    starts = [sum(sizes[:c]) for c in range(len(sizes))]
    left, right = lax.axis_index("left"), lax.axis_index("right")
    ends = [start + size for start, size in zip(starts, sizes)]
    groups = GROUPS if pairs % GROUPS == 0 else 1
    group_y = share_y // groups
    hops_left = sorted(range(1, n_left), key=lambda j: (abs(2 * j - n_left), j))
    hops_right = sorted(range(1, n_right), key=lambda j: (abs(2 * j - n_right), j))

    table_copies = [
        pltpu.make_async_copy(src, dst, sem_t.at[i])
        for i, (src, dst) in enumerate((
            (hx_hbm, hx), (hy_hbm, hy), (wz_hbm, wz), (coup_hbm, coup_ref),
            (sx_hbm, sx_ref), (sy_hbm, sy_ref), (sz_hbm, sz_ref),
        ))
    ]

    def x_copy(pair):
        return pltpu.make_async_copy(
            x_hbm.at[:, pl.ds(2 * pair, 2)], x_buf.at[pair], sem_x.at[pair]
        )

    barrier = pltpu.get_barrier_semaphore()
    for j in hops_left:
        pl.semaphore_signal(
            barrier, inc=1, device_id=(lax.rem(left + j, n_left), right), device_id_type=MESH
        )
    for j in hops_right:
        pl.semaphore_signal(
            barrier, inc=1, device_id=(left, lax.rem(right + j, n_right)), device_id_type=MESH
        )
    table_copies[0].start()
    for pair in range(pairs):
        x_copy(pair).start()
    for copy in table_copies[1:]:
        copy.start()

    def left_copy(chunk, j, first_y=0, count_y=share_y):
        other = lax.rem(left + j, n_left)
        start, size = starts[chunk], sizes[chunk]
        return pltpu.make_async_remote_copy(
            src_ref=send_a.at[
                pl.ds(start * n_left + other * size, size), pl.ds(first_y, count_y)
            ],
            dst_ref=recv_b.at[
                pl.ds(start, size), pl.ds(left * share_y + first_y, count_y)
            ],
            send_sem=sem_as.at[0],
            recv_sem=sem_br.at[chunk],
            device_id=(other, right),
            device_id_type=MESH,
        )

    def right_copy(chunk, j):
        other = lax.rem(right + j, n_right)
        rows = pl.ds(starts[chunk], sizes[chunk])
        return pltpu.make_async_remote_copy(
            src_ref=send_c.at[other, rows],
            dst_ref=recv_d.at[right, rows],
            send_sem=sem_cs.at[0],
            recv_sem=sem_dr.at[chunk],
            device_id=(left, other),
            device_id_type=MESH,
        )

    def wait_bytes(ref, sem):
        pltpu.make_async_copy(ref, ref, sem).wait()

    def left_arrived(chunk):
        rows = pl.ds(starts[chunk], sizes[chunk])
        wait_bytes(recv_b.at[rows, pl.ds(0, (n_left - 1) * share_y)], sem_br.at[chunk])

    def right_arrived(chunk):
        rows = pl.ds(starts[chunk], sizes[chunk])
        wait_bytes(recv_d.at[pl.ds(0, n_right - 1), rows], sem_dr.at[chunk])

    flat_a = send_a.reshape(size_x * share_y, lanes)

    def x_step(pair, carry):
        x_copy(pair).wait()
        planes = [x_buf[pair, :, i].reshape(lanes, size_x) for i in range(2)]
        high, low = split(jnp.concatenate(planes, axis=0))
        dot = functools.partial(
            lax.dot_general,
            dimension_numbers=(((1,), (1,)), ((), ())),
            preferred_element_type=jnp.float32,
        )
        both = dot(hx[...], high)
        modes = both[:size_x] + both[size_x:] + dot(hx[:size_x], low)
        for i in range(2):
            flat_a[pl.ds(2 * pair + i, size_x, stride=share_y), :] = modes[
                :, i * lanes:(i + 1) * lanes
            ]
        return carry

    table_copies[0].wait()
    per_group = pairs // groups
    for group in range(groups):
        lax.fori_loop(group * per_group, (group + 1) * per_group, x_step, 0)
        if group == 0:
            pl.semaphore_wait(barrier, n_left + n_right - 2)
        for j in hops_left:
            left_copy(0, j, group * group_y, group_y).start()

    def left_start(after, upto):
        for chunk in range(1, len(sizes)):
            if after < ends[chunk] <= upto:
                for j in hops_left:
                    left_copy(chunk, j).start()

    left_start(ends[0], max(WINDOW, ends[0]))

    for start, size in zip(starts, sizes):
        recv_b[pl.ds(start, size), pl.ds(left * share_y, share_y)] = send_a[
            pl.ds(start * n_left + left * size, size)
        ]
    for copy in table_copies[1:]:
        copy.wait()
    sy_cols[...] = jnp.broadcast_to(sy_ref[...], (size_z, size_y)).T

    def y_stage(chunk):
        left_arrived(chunk)
        left_start(max(starts[chunk] + WINDOW, ends[0]), ends[chunk] + WINDOW)
        start, size = starts[chunk], sizes[chunk]

        def y_step(step, carry):
            rows = [recv_b[start + 2 * step + i] for i in range(2)]
            high, low = split(jnp.concatenate(rows, axis=1))
            dot = functools.partial(jnp.dot, preferred_element_type=jnp.float32)
            both = dot(hy[...], high)
            modes = both[:size_y] + both[size_y:] + dot(hy[:size_y], low)
            for i in range(2):
                send_c[:, start + 2 * step + i] = modes[:, i * lanes:(i + 1) * lanes].reshape(
                    n_right, block_y, lanes
                )
            return carry

        lax.fori_loop(0, size // 2, y_step, 0)
        for j in hops_right:
            right_copy(chunk, j).start()
        recv_d[right, pl.ds(start, size)] = send_c[right, pl.ds(start, size)]

    def z_stage(chunk):
        right_arrived(chunk)
        start, size = starts[chunk], sizes[chunk]
        count = size * block_y
        lines = [
            recv_d[r, pl.ds(start, size)].reshape(count, lanes) for r in range(n_right)
        ]
        high, low = split(jnp.concatenate(lines, axis=1))
        dot = functools.partial(jnp.dot, preferred_element_type=jnp.float32)
        z_buf[:count] = dot(high, wz[0]) + dot(low, wz[0]) + dot(high, wz[1])

        part_y = sy_cols[pl.ds(pl.multiple_of(right * block_y, block_y), block_y), :]

        def mix_step(step, carry):
            symbol = sx_ref[0, left * block_x + start + step] + part_y + sz_ref[...]
            weight = 1.0 / (1.0 + symbol)
            rest = 1.0 - weight
            rows = pl.ds(pl.multiple_of(step * block_y, block_y), block_y)
            old = [z_buf[rows, b * size_z:(b + 1) * size_z] for b in range(fields)]
            for a in range(fields):
                mixed = coup_ref[a, 0] * old[0]
                for b in range(1, fields):
                    mixed += coup_ref[a, b] * old[b]
                out_ref[a, start + step] = weight * old[a] + rest * mixed
            return carry

        lax.fori_loop(0, size, mix_step, 0)

    for chunk in range(len(sizes)):
        y_stage(chunk)
        if chunk:
            z_stage(chunk - 1)
    z_stage(len(sizes) - 1)

    wait_bytes(send_a.at[pl.ds(0, (n_left - 1) * block_x)], sem_as.at[0])
    wait_bytes(send_c.at[pl.ds(0, n_right - 1)], sem_cs.at[0])


def solution(mesh):
    n_left, n_right = mesh.shape["left"], mesh.shape["right"]

    def body(species, coupling, symbol_x, symbol_y, symbol_z):
        fields, size_x, share_y, share_z = species.shape
        size_y, size_z = symbol_y.shape[0], symbol_z.shape[0]
        lanes = fields * share_z
        block_x, block_y = size_x // n_left, size_y // n_right
        sizes = chunk_sizes(block_x)
        chunks = len(sizes)

        order = np.concatenate([
            np.arange(size_x).reshape(n_left, block_x)[:, sum(sizes[:c]):sum(sizes[:c + 1])].ravel()
            for c in range(chunks)
        ])
        hx = np.concatenate(halves(basis_table(size_x)[order]))
        hy = np.concatenate(halves(basis_table(size_y)))
        hz = basis_table(size_z).reshape(n_right, share_z, size_z)
        wz = np.einsum("rzn,fg->rfzgn", hz, np.eye(fields))
        wz = np.stack(halves(wz.reshape(n_right * lanes, fields * size_z)))

        hbm = pl.BlockSpec(memory_space=pltpu.HBM)
        vmem = pl.BlockSpec(memory_space=pltpu.VMEM)
        f32, bf16 = jnp.float32, jnp.bfloat16
        room = 64 * 2 ** 20 - 2 * (4 * fields * block_x * block_y * size_z)
        return pl.pallas_call(
            functools.partial(kernel, n_left, n_right, sizes),
            out_shape=pltpu.VMEM((fields, block_x, block_y, size_z), f32),
            in_specs=[hbm] * 8,
            out_specs=vmem,
            scratch_shapes=[
                pltpu.VMEM((share_y // 2, fields, 2, share_z, size_x), f32),
                pltpu.VMEM(hx.shape, bf16),
                pltpu.VMEM(hy.shape, bf16),
                pltpu.VMEM(wz.shape, bf16),
                pltpu.SMEM(coupling.shape, f32),
                pltpu.SMEM((1, size_x), f32),
                pltpu.VMEM((1, size_y), f32),
                pltpu.VMEM((1, size_z), f32),
                pltpu.VMEM((size_x, share_y, lanes), f32),
                pltpu.VMEM((block_x, size_y, lanes), f32),
                pltpu.VMEM((n_right, block_x, block_y, lanes), f32),
                pltpu.VMEM((n_right, block_x, block_y, lanes), f32),
                pltpu.VMEM((max(sizes) * block_y, fields * size_z), f32),
                pltpu.VMEM((size_y, size_z), f32),
                pltpu.SemaphoreType.DMA((share_y // 2,)),
                pltpu.SemaphoreType.DMA((7,)),
                pltpu.SemaphoreType.DMA((1,)),
                pltpu.SemaphoreType.DMA((chunks,)),
                pltpu.SemaphoreType.DMA((1,)),
                pltpu.SemaphoreType.DMA((chunks,)),
            ],
            compiler_params=pltpu.CompilerParams(
                collective_id=0, has_side_effects=True, vmem_limit_bytes=room
            ),
        )(
            jnp.transpose(species, (0, 2, 3, 1)), jnp.asarray(hx), jnp.asarray(hy),
            jnp.asarray(wz), coupling, symbol_x[None], symbol_y[None], symbol_z[None],
        )

    in_specs = (P(None, None, "left", "right"), P(), P(), P(), P())
    out_specs = P(None, "left", "right", None)
    return jax.shard_map(body, mesh=mesh, in_specs=in_specs, out_specs=out_specs, check_vma=False)
```

```python
import functools

import jax
import jax.numpy as jnp
import numpy as np
from jax import lax
from jax.experimental import pallas as pl
from jax.experimental.pallas import tpu as pltpu
from jax.sharding import PartitionSpec as P

MESH = pl.DeviceIdType.MESH
INNER = 6
OUTER = 18
PARTS = (4, 4, 4, 4, 4, 4, 4, 2, 2)
GROUPS = (2, 2, 4)
WINDOW = 12
LAG = 2


def chunk_sizes(block):
    unit = block // sum(PARTS)
    return [part * unit for part in PARTS] if unit and block % sum(PARTS) == 0 else [block]


def basis_table(count):
    rank = np.arange(count)
    angle = 2.0 * np.pi / count * (rank[:, None] * rank[None, :] % count)
    return (np.cos(angle) + np.sin(angle)) / np.sqrt(count)


def halves(table):
    table = table.astype(np.float32)
    high = table.astype(jnp.bfloat16)
    low = (table - high.astype(np.float32)).astype(jnp.bfloat16)
    return high, low


def split(values):
    high = values.astype(jnp.bfloat16)
    low = (values - high.astype(jnp.float32)).astype(jnp.bfloat16)
    return high, low


def kernel(
    n_left, n_right, sizes,
    x_hbm, hx_hbm, hy_hbm, wz_hbm, coup_hbm, sx_hbm, sy_hbm, sz_hbm,
    out_ref,
    x_buf, hx, hy, wz, coup_ref, sx_ref, sy_ref, sz_ref, send_a, recv_b, send_c, recv_d, z_buf, sy_cols,
    sem_x, sem_t, sem_as, sem_br, sem_cs, sem_dr, ready,
):
    fields, share_y, share_z, size_x = x_hbm.shape
    size_y, size_z = sy_hbm.shape[1], sz_hbm.shape[1]
    lanes = fields * share_z
    block_x, block_y = size_x // n_left, size_y // n_right
    pairs = share_y // 2
    starts = [sum(sizes[:c]) for c in range(len(sizes))]
    left, right = lax.axis_index("left"), lax.axis_index("right")
    ends = [start + size for start, size in zip(starts, sizes)]
    groups = GROUPS if sum(GROUPS) == pairs else (pairs,)
    half = n_left // 2
    side, local = left // half, lax.rem(left, half)
    near, far = side * half, (1 - side) * half
    across = [far + side * k + (1 - side) * (half - 1 - k) for k in range(half)]
    beside = [near + lax.rem(local + k, half) for k in range(1, half)]
    hops_right = sorted(range(1, n_right), key=lambda j: (abs(2 * j - n_right), j))

    table_copies = [
        pltpu.make_async_copy(src, dst, sem_t.at[i])
        for i, (src, dst) in enumerate((
            (hx_hbm, hx), (hy_hbm, hy), (wz_hbm, wz), (coup_hbm, coup_ref),
            (sx_hbm, sx_ref), (sy_hbm, sy_ref), (sz_hbm, sz_ref),
        ))
    ]

    def x_copy(pair):
        return pltpu.make_async_copy(
            x_hbm.at[:, pl.ds(2 * pair, 2)], x_buf.at[pair], sem_x.at[pair]
        )

    barrier = pltpu.get_barrier_semaphore()
    for other in across:
        pl.semaphore_signal(barrier, inc=1, device_id=(other, right), device_id_type=MESH)
    for k in range(1, half):
        @pl.when(local < k)
        def _():
            pl.semaphore_signal(
                barrier, inc=1, device_id=(near + k, right), device_id_type=MESH
            )
    for j in hops_right:
        pl.semaphore_signal(
            barrier, inc=1, device_id=(left, lax.rem(right + j, n_right)), device_id_type=MESH
        )
    table_copies[0].start()
    for pair in range(pairs):
        x_copy(pair).start()
    for copy in table_copies[1:]:
        copy.start()

    def left_copy(chunk, other, first_y=0, count_y=share_y):
        start, size = starts[chunk], sizes[chunk]
        return pltpu.make_async_remote_copy(
            src_ref=send_a.at[
                pl.ds(start * n_left + other * size, size), pl.ds(first_y, count_y)
            ],
            dst_ref=recv_b.at[left, pl.ds(start, size), pl.ds(first_y, count_y)],
            send_sem=sem_as.at[0],
            recv_sem=sem_br.at[chunk],
            device_id=(other, right),
            device_id_type=MESH,
        )

    def right_copy(chunk, j):
        other = lax.rem(right + j, n_right)
        rows = pl.ds(starts[chunk], sizes[chunk])
        return pltpu.make_async_remote_copy(
            src_ref=send_c.at[other, rows],
            dst_ref=recv_d.at[right, rows],
            send_sem=sem_cs.at[0],
            recv_sem=sem_dr.at[chunk],
            device_id=(left, other),
            device_id_type=MESH,
        )

    def wait_bytes(ref, sem):
        pltpu.make_async_copy(ref, ref, sem).wait()

    def left_arrived(chunk):
        rows = pl.ds(starts[chunk], sizes[chunk])
        wait_bytes(recv_b.at[pl.ds(0, n_left - 1), rows], sem_br.at[chunk])

    def right_arrived(chunk):
        rows = pl.ds(starts[chunk], sizes[chunk])
        wait_bytes(recv_d.at[pl.ds(0, n_right - 1), rows], sem_dr.at[chunk])

    flat_a = send_a.reshape(size_x * share_y, lanes)

    def x_step(pair, carry):
        x_copy(pair).wait()
        planes = [x_buf[pair, :, i].reshape(lanes, size_x) for i in range(2)]
        high, low = split(jnp.concatenate(planes, axis=0))
        dot = functools.partial(
            lax.dot_general,
            dimension_numbers=(((1,), (1,)), ((), ())),
            preferred_element_type=jnp.float32,
        )
        both = dot(hx[...], high)
        modes = both[:size_x] + both[size_x:] + dot(hx[:size_x], low)
        for i in range(2):
            flat_a[pl.ds(2 * pair + i, size_x, stride=share_y), :] = modes[
                :, i * lanes:(i + 1) * lanes
            ]
        return carry

    table_copies[0].wait()
    done = 0
    for count in groups:
        lax.fori_loop(done, done + count, x_step, 0)
        if done == 0:
            pl.semaphore_wait(barrier, half + local + n_right - 1)
        for other in across:
            left_copy(0, other, 2 * done, 2 * count).start()
        if done == 0:
            for k in range(half - 1):
                @pl.when(k < local)
                def _():
                    pl.semaphore_signal(
                        ready, inc=1, device_id=(near + k, right), device_id_type=MESH
                    )
        done += count

    @pl.when(local < half - 1)
    def _():
        pl.semaphore_wait(ready, half - 1 - local)

    for other in beside:
        left_copy(0, other).start()

    def left_advance(before, now):
        for chunk in range(1, len(sizes)):
            if before + WINDOW < ends[chunk] <= now + WINDOW:
                for other in across + beside:
                    left_copy(chunk, other).start()

    left_advance(-block_x, 0)

    for start, size in zip(starts, sizes):
        recv_b[left, pl.ds(start, size)] = send_a[pl.ds(start * n_left + left * size, size)]
    for copy in table_copies[1:]:
        copy.wait()
    sy_cols[...] = jnp.broadcast_to(sy_ref[...], (size_z, size_y)).T

    def y_stage(chunk):
        left_arrived(chunk)
        left_advance(starts[chunk], ends[chunk])
        start, size = starts[chunk], sizes[chunk]

        def y_step(step, carry):
            rows = [recv_b[:, start + 2 * step + i].reshape(size_y, lanes) for i in range(2)]
            high, low = split(jnp.concatenate(rows, axis=1))
            dot = functools.partial(jnp.dot, preferred_element_type=jnp.float32)
            both = dot(hy[...], high)
            modes = both[:size_y] + both[size_y:] + dot(hy[:size_y], low)
            for i in range(2):
                send_c[:, start + 2 * step + i] = modes[:, i * lanes:(i + 1) * lanes].reshape(
                    n_right, block_y, lanes
                )
            return carry

        lax.fori_loop(0, size // 2, y_step, 0)
        for j in hops_right:
            right_copy(chunk, j).start()
        recv_d[right, pl.ds(start, size)] = send_c[right, pl.ds(start, size)]

    def z_stage(chunk):
        right_arrived(chunk)
        start, size = starts[chunk], sizes[chunk]
        count = size * block_y
        lines = [
            recv_d[r, pl.ds(start, size)].reshape(count, lanes) for r in range(n_right)
        ]
        high, low = split(jnp.concatenate(lines, axis=1))
        dot = functools.partial(jnp.dot, preferred_element_type=jnp.float32)
        both = dot(jnp.concatenate([high, low], axis=0), wz[0])
        z_buf[:count] = both[:count] + both[count:] + dot(high, wz[1])

        part_y = sy_cols[pl.ds(pl.multiple_of(right * block_y, block_y), block_y), :]

        def mix_step(step, carry):
            symbol = sx_ref[0, left * block_x + start + step] + part_y + sz_ref[...]
            weight = 1.0 / (1.0 + symbol)
            rest = 1.0 - weight
            rows = pl.ds(pl.multiple_of(step * block_y, block_y), block_y)
            old = [z_buf[rows, b * size_z:(b + 1) * size_z] for b in range(fields)]
            for a in range(fields):
                mixed = coup_ref[a, 0] * old[0]
                for b in range(1, fields):
                    mixed += coup_ref[a, b] * old[b]
                out_ref[a, start + step] = weight * old[a] + rest * mixed
            return carry

        lax.fori_loop(0, size, mix_step, 0)

    for chunk in range(len(sizes)):
        y_stage(chunk)
        if chunk >= LAG:
            z_stage(chunk - LAG)
    for chunk in range(max(len(sizes) - LAG, 0), len(sizes)):
        z_stage(chunk)

    wait_bytes(send_a.at[pl.ds(0, (n_left - 1) * block_x)], sem_as.at[0])
    wait_bytes(send_c.at[pl.ds(0, n_right - 1)], sem_cs.at[0])


def solution(mesh):
    n_left, n_right = mesh.shape["left"], mesh.shape["right"]

    def body(species, coupling, symbol_x, symbol_y, symbol_z):
        fields, size_x, share_y, share_z = species.shape
        size_y, size_z = symbol_y.shape[0], symbol_z.shape[0]
        lanes = fields * share_z
        block_x, block_y = size_x // n_left, size_y // n_right
        sizes = chunk_sizes(block_x)
        chunks = len(sizes)

        order = np.concatenate([
            np.arange(size_x).reshape(n_left, block_x)[:, sum(sizes[:c]):sum(sizes[:c + 1])].ravel()
            for c in range(chunks)
        ])
        hx = np.concatenate(halves(basis_table(size_x)[order]))
        hy = np.concatenate(halves(basis_table(size_y)))
        hz = basis_table(size_z).reshape(n_right, share_z, size_z)
        wz = np.einsum("rzn,fg->rfzgn", hz, np.eye(fields))
        wz = np.stack(halves(wz.reshape(n_right * lanes, fields * size_z)))

        hbm = pl.BlockSpec(memory_space=pltpu.HBM)
        vmem = pl.BlockSpec(memory_space=pltpu.VMEM)
        f32, bf16 = jnp.float32, jnp.bfloat16
        room = 64 * 2 ** 20 - 2 * (4 * fields * block_x * block_y * size_z)
        return pl.pallas_call(
            functools.partial(kernel, n_left, n_right, sizes),
            out_shape=pltpu.VMEM((fields, block_x, block_y, size_z), f32),
            in_specs=[hbm] * 8,
            out_specs=vmem,
            scratch_shapes=[
                pltpu.VMEM((share_y // 2, fields, 2, share_z, size_x), f32),
                pltpu.VMEM(hx.shape, bf16),
                pltpu.VMEM(hy.shape, bf16),
                pltpu.VMEM(wz.shape, bf16),
                pltpu.SMEM(coupling.shape, f32),
                pltpu.SMEM((1, size_x), f32),
                pltpu.VMEM((1, size_y), f32),
                pltpu.VMEM((1, size_z), f32),
                pltpu.VMEM((size_x, share_y, lanes), f32),
                pltpu.VMEM((n_left, block_x, share_y, lanes), f32),
                pltpu.VMEM((n_right, block_x, block_y, lanes), f32),
                pltpu.VMEM((n_right, block_x, block_y, lanes), f32),
                pltpu.VMEM((max(sizes) * block_y, fields * size_z), f32),
                pltpu.VMEM((size_y, size_z), f32),
                pltpu.SemaphoreType.DMA((share_y // 2,)),
                pltpu.SemaphoreType.DMA((7,)),
                pltpu.SemaphoreType.DMA((1,)),
                pltpu.SemaphoreType.DMA((chunks,)),
                pltpu.SemaphoreType.DMA((1,)),
                pltpu.SemaphoreType.DMA((chunks,)),
                pltpu.SemaphoreType.REGULAR,
            ],
            compiler_params=pltpu.CompilerParams(
                collective_id=0, has_side_effects=True, vmem_limit_bytes=room
            ),
        )(
            jnp.transpose(species, (0, 2, 3, 1)), jnp.asarray(hx), jnp.asarray(hy),
            jnp.asarray(wz), coupling, symbol_x[None], symbol_y[None], symbol_z[None],
        )

    in_specs = (P(None, None, "left", "right"), P(), P(), P(), P())
    out_specs = P(None, "left", "right", None)
    return jax.shard_map(body, mesh=mesh, in_specs=in_specs, out_specs=out_specs, check_vma=False)
```

```python
import functools

import jax
import jax.numpy as jnp
import numpy as np
from jax import lax
from jax.experimental import pallas as pl
from jax.experimental.pallas import tpu as pltpu
from jax.sharding import PartitionSpec as P

MESH = pl.DeviceIdType.MESH
INNER = 6
OUTER = 18
PARTS = (4, 4, 4, 4, 4, 4, 4, 2, 2)
GROUPS = (2, 2, 4)
WINDOW = 12
TAIL = 2
BACK = 8
WIDE = 2
LAG = 2


def chunk_sizes(block):
    unit = block // sum(PARTS)
    return [part * unit for part in PARTS] if unit and block % sum(PARTS) == 0 else [block]


def basis_table(count):
    rank = np.arange(count)
    angle = 2.0 * np.pi / count * (rank[:, None] * rank[None, :] % count)
    return (np.cos(angle) + np.sin(angle)) / np.sqrt(count)


def halves(table):
    table = table.astype(np.float32)
    high = table.astype(jnp.bfloat16)
    low = (table - high.astype(np.float32)).astype(jnp.bfloat16)
    return high, low


def split(values):
    high = values.astype(jnp.bfloat16)
    low = (values - high.astype(jnp.float32)).astype(jnp.bfloat16)
    return high, low


def kernel(
    n_left, n_right, sizes,
    x_hbm, hx_hbm, hy_hbm, wz_hbm, coup_hbm, sx_hbm, sy_hbm, sz_hbm,
    out_ref,
    x_buf, hx, hy, wz, coup_ref, sx_ref, sy_ref, sz_ref, send_a, recv_b, send_c, recv_d, z_buf, sy_cols,
    sem_x, sem_t, sem_as, sem_br, sem_cs, sem_dr, ready,
):
    fields, share_y, share_z, size_x = x_hbm.shape
    size_y, size_z = sy_hbm.shape[1], sz_hbm.shape[1]
    lanes = fields * share_z
    block_x, block_y = size_x // n_left, size_y // n_right
    pairs = share_y // 2
    starts = [sum(sizes[:c]) for c in range(len(sizes))]
    left, right = lax.axis_index("left"), lax.axis_index("right")
    ends = [start + size for start, size in zip(starts, sizes)]
    groups = GROUPS if sum(GROUPS) == pairs else (pairs,)
    half = n_left // 2
    side, local = left // half, lax.rem(left, half)
    near, far = side * half, (1 - side) * half
    across = [far + side * k + (1 - side) * (half - 1 - k) for k in range(half)]
    beside = [near + lax.rem(local + k, half) for k in range(1, half)]
    hops_right = sorted(range(1, n_right), key=lambda j: (abs(2 * j - n_right), j))

    table_copies = [
        pltpu.make_async_copy(src, dst, sem_t.at[i])
        for i, (src, dst) in enumerate((
            (hx_hbm, hx), (hy_hbm, hy), (wz_hbm, wz), (coup_hbm, coup_ref),
            (sx_hbm, sx_ref), (sy_hbm, sy_ref), (sz_hbm, sz_ref),
        ))
    ]

    def x_copy(pair):
        return pltpu.make_async_copy(
            x_hbm.at[:, pl.ds(2 * pair, 2)], x_buf.at[pair], sem_x.at[pair]
        )

    barrier = pltpu.get_barrier_semaphore()
    for other in across:
        pl.semaphore_signal(barrier, inc=1, device_id=(other, right), device_id_type=MESH)
    for k in range(1, half):
        @pl.when(local < k)
        def _():
            pl.semaphore_signal(
                barrier, inc=1, device_id=(near + k, right), device_id_type=MESH
            )
    for j in hops_right:
        pl.semaphore_signal(
            barrier, inc=1, device_id=(left, lax.rem(right + j, n_right)), device_id_type=MESH
        )
    table_copies[0].start()
    for pair in range(pairs):
        x_copy(pair).start()
    for copy in table_copies[1:]:
        copy.start()

    def left_copy(chunk, other, first_y=0, count_y=share_y):
        start, size = starts[chunk], sizes[chunk]
        return pltpu.make_async_remote_copy(
            src_ref=send_a.at[
                pl.ds(start * n_left + other * size, size), pl.ds(first_y, count_y)
            ],
            dst_ref=recv_b.at[left, pl.ds(start, size), pl.ds(first_y, count_y)],
            send_sem=sem_as.at[0],
            recv_sem=sem_br.at[chunk],
            device_id=(other, right),
            device_id_type=MESH,
        )

    def right_copy(chunk, j):
        other = lax.rem(right + j, n_right)
        rows = pl.ds(starts[chunk], sizes[chunk])
        return pltpu.make_async_remote_copy(
            src_ref=send_c.at[other, rows],
            dst_ref=recv_d.at[right, rows],
            send_sem=sem_cs.at[0],
            recv_sem=sem_dr.at[chunk],
            device_id=(left, other),
            device_id_type=MESH,
        )

    def wait_bytes(ref, sem):
        pltpu.make_async_copy(ref, ref, sem).wait()

    def left_arrived(chunk):
        rows = pl.ds(starts[chunk], sizes[chunk])
        wait_bytes(recv_b.at[pl.ds(0, n_left - 1), rows], sem_br.at[chunk])

    def right_arrived(chunk):
        rows = pl.ds(starts[chunk], sizes[chunk])
        wait_bytes(recv_d.at[pl.ds(0, n_right - 1), rows], sem_dr.at[chunk])

    flat_a = send_a.reshape(size_x * share_y, lanes)

    wide = WIDE if all(count % WIDE == 0 for count in groups) else 1

    def x_step(step, carry):
        planes = []
        for i in range(wide):
            x_copy(step * wide + i).wait()
            planes += [x_buf[step * wide + i, :, k].reshape(lanes, size_x) for k in range(2)]
        high, low = split(jnp.concatenate(planes, axis=0))
        dot = functools.partial(
            lax.dot_general,
            dimension_numbers=(((1,), (1,)), ((), ())),
            preferred_element_type=jnp.float32,
        )
        both = dot(hx[...], high)
        modes = both[:size_x] + both[size_x:] + dot(hx[:size_x], low)
        for i in range(2 * wide):
            flat_a[pl.ds(2 * wide * step + i, size_x, stride=share_y), :] = modes[
                :, i * lanes:(i + 1) * lanes
            ]
        return carry

    table_copies[0].wait()
    done = 0
    for count in groups:
        lax.fori_loop(done // wide, (done + count) // wide, x_step, 0)
        if done == 0:
            pl.semaphore_wait(barrier, half + local + n_right - 1)
        for other in across:
            left_copy(0, other, 2 * done, 2 * count).start()
        if done == 0:
            for k in range(half - 1):
                @pl.when(k < local)
                def _():
                    pl.semaphore_signal(
                        ready, inc=1, device_id=(near + k, right), device_id_type=MESH
                    )
        done += count

    @pl.when(local < half - 1)
    def _():
        pl.semaphore_wait(ready, half - 1 - local)

    for other in beside:
        left_copy(0, other).start()

    def left_advance(before, now):
        for chunk in range(1, len(sizes)):
            if before + WINDOW < ends[chunk] <= now + WINDOW:
                left_copy(chunk, across[0]).start()
            window = WINDOW if chunk < len(sizes) - TAIL else BACK
            if before + window < ends[chunk] <= now + window:
                for other in across[1:] + beside:
                    left_copy(chunk, other).start()

    left_advance(-block_x, 0)

    for start, size in zip(starts, sizes):
        recv_b[left, pl.ds(start, size)] = send_a[pl.ds(start * n_left + left * size, size)]
    for copy in table_copies[1:]:
        copy.wait()
    sy_cols[...] = jnp.broadcast_to(sy_ref[...], (size_z, size_y)).T

    def y_stage(chunk):
        left_arrived(chunk)
        left_advance(starts[chunk], ends[chunk])
        start, size = starts[chunk], sizes[chunk]

        def y_step(step, carry):
            rows = [recv_b[:, start + 2 * step + i].reshape(size_y, lanes) for i in range(2)]
            high, low = split(jnp.concatenate(rows, axis=1))
            dot = functools.partial(jnp.dot, preferred_element_type=jnp.float32)
            both = dot(hy[...], high)
            modes = both[:size_y] + both[size_y:] + dot(hy[:size_y], low)
            for i in range(2):
                send_c[:, start + 2 * step + i] = modes[:, i * lanes:(i + 1) * lanes].reshape(
                    n_right, block_y, lanes
                )
            return carry

        lax.fori_loop(0, size // 2, y_step, 0)
        for j in hops_right:
            right_copy(chunk, j).start()
        recv_d[right, pl.ds(start, size)] = send_c[right, pl.ds(start, size)]

    def z_stage(chunk):
        right_arrived(chunk)
        start, size = starts[chunk], sizes[chunk]
        count = size * block_y
        lines = [
            recv_d[r, pl.ds(start, size)].reshape(count, lanes) for r in range(n_right)
        ]
        high, low = split(jnp.concatenate(lines, axis=1))
        dot = functools.partial(jnp.dot, preferred_element_type=jnp.float32)
        both = dot(jnp.concatenate([high, low], axis=0), wz[0])
        z_buf[:count] = both[:count] + both[count:] + dot(high, wz[1])

        part_y = sy_cols[pl.ds(pl.multiple_of(right * block_y, block_y), block_y), :]

        def mix_step(step, carry):
            symbol = sx_ref[0, left * block_x + start + step] + part_y + sz_ref[...]
            weight = 1.0 / (1.0 + symbol)
            rest = 1.0 - weight
            rows = pl.ds(pl.multiple_of(step * block_y, block_y), block_y)
            old = [z_buf[rows, b * size_z:(b + 1) * size_z] for b in range(fields)]
            for a in range(fields):
                mixed = coup_ref[a, 0] * old[0]
                for b in range(1, fields):
                    mixed += coup_ref[a, b] * old[b]
                out_ref[a, start + step] = weight * old[a] + rest * mixed
            return carry

        lax.fori_loop(0, size, mix_step, 0)

    for chunk in range(len(sizes)):
        y_stage(chunk)
        if chunk >= LAG:
            z_stage(chunk - LAG)
    for chunk in range(max(len(sizes) - LAG, 0), len(sizes)):
        z_stage(chunk)

    wait_bytes(send_a.at[pl.ds(0, (n_left - 1) * block_x)], sem_as.at[0])
    wait_bytes(send_c.at[pl.ds(0, n_right - 1)], sem_cs.at[0])


def solution(mesh):
    n_left, n_right = mesh.shape["left"], mesh.shape["right"]

    def body(species, coupling, symbol_x, symbol_y, symbol_z):
        fields, size_x, share_y, share_z = species.shape
        size_y, size_z = symbol_y.shape[0], symbol_z.shape[0]
        lanes = fields * share_z
        block_x, block_y = size_x // n_left, size_y // n_right
        sizes = chunk_sizes(block_x)
        chunks = len(sizes)

        order = np.concatenate([
            np.arange(size_x).reshape(n_left, block_x)[:, sum(sizes[:c]):sum(sizes[:c + 1])].ravel()
            for c in range(chunks)
        ])
        hx = np.concatenate(halves(basis_table(size_x)[order]))
        hy = np.concatenate(halves(basis_table(size_y)))
        hz = basis_table(size_z).reshape(n_right, share_z, size_z)
        wz = np.einsum("rzn,fg->rfzgn", hz, np.eye(fields))
        wz = np.stack(halves(wz.reshape(n_right * lanes, fields * size_z)))

        hbm = pl.BlockSpec(memory_space=pltpu.HBM)
        vmem = pl.BlockSpec(memory_space=pltpu.VMEM)
        f32, bf16 = jnp.float32, jnp.bfloat16
        room = 64 * 2 ** 20 - 2 * (4 * fields * block_x * block_y * size_z)
        return pl.pallas_call(
            functools.partial(kernel, n_left, n_right, sizes),
            out_shape=pltpu.VMEM((fields, block_x, block_y, size_z), f32),
            in_specs=[hbm] * 8,
            out_specs=vmem,
            scratch_shapes=[
                pltpu.VMEM((share_y // 2, fields, 2, share_z, size_x), f32),
                pltpu.VMEM(hx.shape, bf16),
                pltpu.VMEM(hy.shape, bf16),
                pltpu.VMEM(wz.shape, bf16),
                pltpu.SMEM(coupling.shape, f32),
                pltpu.SMEM((1, size_x), f32),
                pltpu.VMEM((1, size_y), f32),
                pltpu.VMEM((1, size_z), f32),
                pltpu.VMEM((size_x, share_y, lanes), f32),
                pltpu.VMEM((n_left, block_x, share_y, lanes), f32),
                pltpu.VMEM((n_right, block_x, block_y, lanes), f32),
                pltpu.VMEM((n_right, block_x, block_y, lanes), f32),
                pltpu.VMEM((max(sizes) * block_y, fields * size_z), f32),
                pltpu.VMEM((size_y, size_z), f32),
                pltpu.SemaphoreType.DMA((share_y // 2,)),
                pltpu.SemaphoreType.DMA((7,)),
                pltpu.SemaphoreType.DMA((1,)),
                pltpu.SemaphoreType.DMA((chunks,)),
                pltpu.SemaphoreType.DMA((1,)),
                pltpu.SemaphoreType.DMA((chunks,)),
                pltpu.SemaphoreType.REGULAR,
            ],
            compiler_params=pltpu.CompilerParams(
                collective_id=0, has_side_effects=True, vmem_limit_bytes=room
            ),
        )(
            jnp.transpose(species, (0, 2, 3, 1)), jnp.asarray(hx), jnp.asarray(hy),
            jnp.asarray(wz), coupling, symbol_x[None], symbol_y[None], symbol_z[None],
        )

    in_specs = (P(None, None, "left", "right"), P(), P(), P(), P())
    out_specs = P(None, "left", "right", None)
    return jax.shard_map(body, mesh=mesh, in_specs=in_specs, out_specs=out_specs, check_vma=False)
```

```python
import functools

import jax
import jax.numpy as jnp
import numpy as np
from jax import lax
from jax.experimental import pallas as pl
from jax.experimental.pallas import tpu as pltpu
from jax.sharding import PartitionSpec as P

MESH = pl.DeviceIdType.MESH
INNER = 6
OUTER = 18
PARTS = (4, 4, 4, 4, 4, 4, 4, 2, 2)
GROUPS = (2, 2, 4)
WINDOW = 12
TAIL = 2
BACK = 8
WIDE = 2
TALL = 4
LAG = 2
HOLD = 3


def chunk_sizes(block):
    unit = block // sum(PARTS)
    return [part * unit for part in PARTS] if unit and block % sum(PARTS) == 0 else [block]


def basis_table(count):
    rank = np.arange(count)
    angle = 2.0 * np.pi / count * (rank[:, None] * rank[None, :] % count)
    return (np.cos(angle) + np.sin(angle)) / np.sqrt(count)


def halves(table):
    table = table.astype(np.float32)
    high = table.astype(jnp.bfloat16)
    low = (table - high.astype(np.float32)).astype(jnp.bfloat16)
    return high, low


def split(values):
    high = values.astype(jnp.bfloat16)
    low = (values - high.astype(jnp.float32)).astype(jnp.bfloat16)
    return high, low


def kernel(
    n_left, n_right, sizes,
    x_hbm, hx_hbm, hy_hbm, wz_hbm, coup_hbm, sx_hbm, sy_hbm, sz_hbm,
    out_ref,
    x_buf, hx, hy, wz, coup_ref, sx_ref, sy_ref, sz_ref, send_a, recv_b, send_c, recv_d, z_buf, sy_cols,
    sem_x, sem_t, sem_as, sem_br, sem_cs, sem_dr, ready,
):
    fields, share_y, share_z, size_x = x_hbm.shape
    size_y, size_z = sy_hbm.shape[1], sz_hbm.shape[1]
    lanes = fields * share_z
    block_x, block_y = size_x // n_left, size_y // n_right
    pairs = share_y // 2
    starts = [sum(sizes[:c]) for c in range(len(sizes))]
    left, right = lax.axis_index("left"), lax.axis_index("right")
    ends = [start + size for start, size in zip(starts, sizes)]
    groups = GROUPS if sum(GROUPS) == pairs else (pairs,)
    half = n_left // 2
    side, local = left // half, lax.rem(left, half)
    near, far = side * half, (1 - side) * half
    across = [far + side * k + (1 - side) * (half - 1 - k) for k in range(half)]
    beside = [near + lax.rem(local + k, half) for k in range(1, half)]
    hops_right = sorted(range(1, n_right), key=lambda j: (abs(2 * j - n_right), j))

    table_copies = [
        pltpu.make_async_copy(src, dst, sem_t.at[i])
        for i, (src, dst) in enumerate((
            (hx_hbm, hx), (hy_hbm, hy), (wz_hbm, wz), (coup_hbm, coup_ref),
            (sx_hbm, sx_ref), (sy_hbm, sy_ref), (sz_hbm, sz_ref),
        ))
    ]

    def x_copy(pair):
        return pltpu.make_async_copy(
            x_hbm.at[:, pl.ds(2 * pair, 2)], x_buf.at[pair], sem_x.at[pair]
        )

    barrier = pltpu.get_barrier_semaphore()
    for other in across:
        pl.semaphore_signal(barrier, inc=1, device_id=(other, right), device_id_type=MESH)
    for k in range(1, half):
        @pl.when(local < k)
        def _():
            pl.semaphore_signal(
                barrier, inc=1, device_id=(near + k, right), device_id_type=MESH
            )
    for j in hops_right:
        pl.semaphore_signal(
            barrier, inc=1, device_id=(left, lax.rem(right + j, n_right)), device_id_type=MESH
        )
    table_copies[0].start()
    for pair in range(pairs):
        x_copy(pair).start()
    for copy in table_copies[1:]:
        copy.start()

    def left_copy(chunk, other, first_y=0, count_y=share_y):
        start, size = starts[chunk], sizes[chunk]
        return pltpu.make_async_remote_copy(
            src_ref=send_a.at[
                pl.ds(start * n_left + other * size, size), pl.ds(first_y, count_y)
            ],
            dst_ref=recv_b.at[left, pl.ds(start, size), pl.ds(first_y, count_y)],
            send_sem=sem_as.at[0],
            recv_sem=sem_br.at[chunk],
            device_id=(other, right),
            device_id_type=MESH,
        )

    def right_copy(chunk, j):
        other = lax.rem(right + j, n_right)
        rows = pl.ds(starts[chunk], sizes[chunk])
        return pltpu.make_async_remote_copy(
            src_ref=send_c.at[other, rows],
            dst_ref=recv_d.at[right, rows],
            send_sem=sem_cs.at[0],
            recv_sem=sem_dr.at[chunk],
            device_id=(left, other),
            device_id_type=MESH,
        )

    def wait_bytes(ref, sem):
        pltpu.make_async_copy(ref, ref, sem).wait()

    def left_arrived(chunk):
        rows = pl.ds(starts[chunk], sizes[chunk])
        wait_bytes(recv_b.at[pl.ds(0, n_left - 1), rows], sem_br.at[chunk])

    def right_arrived(chunk):
        rows = pl.ds(starts[chunk], sizes[chunk])
        wait_bytes(recv_d.at[pl.ds(0, n_right - 1), rows], sem_dr.at[chunk])

    flat_a = send_a.reshape(size_x * share_y, lanes)

    wide = WIDE if all(count % WIDE == 0 for count in groups) else 1

    def x_step(step, carry):
        planes = []
        for i in range(wide):
            x_copy(step * wide + i).wait()
            planes += [x_buf[step * wide + i, :, k].reshape(lanes, size_x) for k in range(2)]
        high, low = split(jnp.concatenate(planes, axis=0))
        dot = functools.partial(
            lax.dot_general,
            dimension_numbers=(((1,), (1,)), ((), ())),
            preferred_element_type=jnp.float32,
        )
        both = dot(hx[...], high)
        modes = both[:size_x] + both[size_x:] + dot(hx[:size_x], low)
        for i in range(2 * wide):
            flat_a[pl.ds(2 * wide * step + i, size_x, stride=share_y), :] = modes[
                :, i * lanes:(i + 1) * lanes
            ]
        return carry

    table_copies[0].wait()
    done = 0
    for count in groups:
        lax.fori_loop(done // wide, (done + count) // wide, x_step, 0)
        if done == 0:
            pl.semaphore_wait(barrier, half + local + n_right - 1)
        for other in across:
            left_copy(0, other, 2 * done, 2 * count).start()
        if done == 0:
            for k in range(half - 1):
                @pl.when(k < local)
                def _():
                    pl.semaphore_signal(
                        ready, inc=1, device_id=(near + k, right), device_id_type=MESH
                    )
        done += count

    @pl.when(local < half - 1)
    def _():
        pl.semaphore_wait(ready, half - 1 - local)

    for other in beside:
        left_copy(0, other).start()

    def left_advance(before, now):
        for chunk in range(1, len(sizes)):
            if before + WINDOW < ends[chunk] <= now + WINDOW:
                left_copy(chunk, across[0]).start()
            window = BACK if chunk >= len(sizes) - TAIL else WINDOW
            if before + window < ends[chunk] <= now + window:
                for other in across[1:] + beside:
                    left_copy(chunk, other).start()

    left_advance(-block_x, 0)

    for start, size in zip(starts, sizes):
        recv_b[left, pl.ds(start, size)] = send_a[pl.ds(start * n_left + left * size, size)]
    for copy in table_copies[1:]:
        copy.wait()
    sy_cols[...] = jnp.broadcast_to(sy_ref[...], (size_z, size_y)).T

    def y_stage(chunk):
        left_arrived(chunk)
        left_advance(starts[chunk], ends[chunk])
        start, size = starts[chunk], sizes[chunk]

        tall = TALL if size % TALL == 0 else 2

        def y_step(step, carry):
            first = start + tall * step
            rows = [recv_b[:, first + i].reshape(size_y, lanes) for i in range(tall)]
            high, low = split(jnp.concatenate(rows, axis=1))
            dot = functools.partial(jnp.dot, preferred_element_type=jnp.float32)
            both = dot(hy[...], high)
            modes = both[:size_y] + both[size_y:] + dot(hy[:size_y], low)
            for i in range(tall):
                send_c[:, first + i] = modes[:, i * lanes:(i + 1) * lanes].reshape(
                    n_right, block_y, lanes
                )
            return carry

        lax.fori_loop(0, size // tall, y_step, 0)
        for j in hops_right:
            right_copy(chunk, j).start()
        recv_d[right, pl.ds(start, size)] = send_c[right, pl.ds(start, size)]

    def z_stage(chunk):
        right_arrived(chunk)
        start, size = starts[chunk], sizes[chunk]
        count = size * block_y
        lines = [
            recv_d[r, pl.ds(start, size)].reshape(count, lanes) for r in range(n_right)
        ]
        high, low = split(jnp.concatenate(lines, axis=1))
        dot = functools.partial(jnp.dot, preferred_element_type=jnp.float32)
        both = dot(jnp.concatenate([high, low], axis=0), wz[0])
        z_buf[:count] = both[:count] + both[count:] + dot(high, wz[1])

        part_y = sy_cols[pl.ds(pl.multiple_of(right * block_y, block_y), block_y), :]

        def mix_step(step, carry):
            symbol = sx_ref[0, left * block_x + start + step] + part_y + sz_ref[...]
            weight = 1.0 / (1.0 + symbol)
            rest = 1.0 - weight
            rows = pl.ds(pl.multiple_of(step * block_y, block_y), block_y)
            old = [z_buf[rows, b * size_z:(b + 1) * size_z] for b in range(fields)]
            for a in range(fields):
                mixed = coup_ref[a, 0] * old[0]
                for b in range(1, fields):
                    mixed += coup_ref[a, b] * old[b]
                out_ref[a, start + step] = weight * old[a] + rest * mixed
            return carry

        lax.fori_loop(0, size, mix_step, 0)

    for chunk in range(len(sizes)):
        y_stage(chunk)
        if LAG <= chunk < len(sizes) - HOLD:
            z_stage(chunk - LAG)
    for chunk in range(max(len(sizes) - HOLD - LAG, 0), len(sizes)):
        z_stage(chunk)

    wait_bytes(send_a.at[pl.ds(0, (n_left - 1) * block_x)], sem_as.at[0])
    wait_bytes(send_c.at[pl.ds(0, n_right - 1)], sem_cs.at[0])


def solution(mesh):
    n_left, n_right = mesh.shape["left"], mesh.shape["right"]

    def body(species, coupling, symbol_x, symbol_y, symbol_z):
        fields, size_x, share_y, share_z = species.shape
        size_y, size_z = symbol_y.shape[0], symbol_z.shape[0]
        lanes = fields * share_z
        block_x, block_y = size_x // n_left, size_y // n_right
        sizes = chunk_sizes(block_x)
        chunks = len(sizes)

        order = np.concatenate([
            np.arange(size_x).reshape(n_left, block_x)[:, sum(sizes[:c]):sum(sizes[:c + 1])].ravel()
            for c in range(chunks)
        ])
        hx = np.concatenate(halves(basis_table(size_x)[order]))
        hy = np.concatenate(halves(basis_table(size_y)))
        hz = basis_table(size_z).reshape(n_right, share_z, size_z)
        wz = np.einsum("rzn,fg->rfzgn", hz, np.eye(fields))
        wz = np.stack(halves(wz.reshape(n_right * lanes, fields * size_z)))

        hbm = pl.BlockSpec(memory_space=pltpu.HBM)
        vmem = pl.BlockSpec(memory_space=pltpu.VMEM)
        f32, bf16 = jnp.float32, jnp.bfloat16
        room = 64 * 2 ** 20 - 2 * (4 * fields * block_x * block_y * size_z)
        return pl.pallas_call(
            functools.partial(kernel, n_left, n_right, sizes),
            out_shape=pltpu.VMEM((fields, block_x, block_y, size_z), f32),
            in_specs=[hbm] * 8,
            out_specs=vmem,
            scratch_shapes=[
                pltpu.VMEM((share_y // 2, fields, 2, share_z, size_x), f32),
                pltpu.VMEM(hx.shape, bf16),
                pltpu.VMEM(hy.shape, bf16),
                pltpu.VMEM(wz.shape, bf16),
                pltpu.SMEM(coupling.shape, f32),
                pltpu.SMEM((1, size_x), f32),
                pltpu.VMEM((1, size_y), f32),
                pltpu.VMEM((1, size_z), f32),
                pltpu.VMEM((size_x, share_y, lanes), f32),
                pltpu.VMEM((n_left, block_x, share_y, lanes), f32),
                pltpu.VMEM((n_right, block_x, block_y, lanes), f32),
                pltpu.VMEM((n_right, block_x, block_y, lanes), f32),
                pltpu.VMEM((max(sizes) * block_y, fields * size_z), f32),
                pltpu.VMEM((size_y, size_z), f32),
                pltpu.SemaphoreType.DMA((share_y // 2,)),
                pltpu.SemaphoreType.DMA((7,)),
                pltpu.SemaphoreType.DMA((1,)),
                pltpu.SemaphoreType.DMA((chunks,)),
                pltpu.SemaphoreType.DMA((1,)),
                pltpu.SemaphoreType.DMA((chunks,)),
                pltpu.SemaphoreType.REGULAR,
            ],
            compiler_params=pltpu.CompilerParams(
                collective_id=0, has_side_effects=True, vmem_limit_bytes=room
            ),
        )(
            jnp.transpose(species, (0, 2, 3, 1)), jnp.asarray(hx), jnp.asarray(hy),
            jnp.asarray(wz), coupling, symbol_x[None], symbol_y[None], symbol_z[None],
        )

    in_specs = (P(None, None, "left", "right"), P(), P(), P(), P())
    out_specs = P(None, "left", "right", None)
    return jax.shard_map(body, mesh=mesh, in_specs=in_specs, out_specs=out_specs, check_vma=False)
```

```python
import functools

import jax
import jax.numpy as jnp
import numpy as np
from jax import lax
from jax.experimental import pallas as pl
from jax.experimental.pallas import tpu as pltpu
from jax.sharding import PartitionSpec as P

MESH = pl.DeviceIdType.MESH
PARTS = (4, 4, 4, 4, 4, 4, 2, 2, 2, 2)
GROUPS = (2, 2, 4)
WINDOW = 12
TAIL = 2
BACK = 6
WIDE = 2
TALL = 4
LAG = 2
HOLD = 3


def chunk_sizes(block):
    unit = block // sum(PARTS)
    return [part * unit for part in PARTS] if unit and block % sum(PARTS) == 0 else [block]


def basis_table(count):
    rank = np.arange(count)
    angle = 2.0 * np.pi / count * (rank[:, None] * rank[None, :] % count)
    return (np.cos(angle) + np.sin(angle)) / np.sqrt(count)


def halves(table):
    table = table.astype(np.float32)
    high = table.astype(jnp.bfloat16)
    low = (table - high.astype(np.float32)).astype(jnp.bfloat16)
    return high, low


def split(values):
    high = values.astype(jnp.bfloat16)
    low = (values - high.astype(jnp.float32)).astype(jnp.bfloat16)
    return high, low


def kernel(
    n_left, n_right, sizes,
    x_hbm, hx_hbm, hy_hbm, wz_hbm, coup_hbm, sx_hbm, sy_hbm, sz_hbm,
    out_ref,
    x_buf, hx, hy, wz, coup_ref, sx_ref, sy_ref, sz_ref, send_a, recv_b, send_c, recv_d, z_buf, sy_cols,
    sem_x, sem_t, sem_as, sem_br, sem_cs, sem_dr, ready,
):
    fields, share_y, share_z, size_x = x_hbm.shape
    size_y, size_z = sy_hbm.shape[1], sz_hbm.shape[1]
    lanes = fields * share_z
    block_x, block_y = size_x // n_left, size_y // n_right
    pairs = share_y // 2
    starts = [sum(sizes[:c]) for c in range(len(sizes))]
    left, right = lax.axis_index("left"), lax.axis_index("right")
    ends = [start + size for start, size in zip(starts, sizes)]
    groups = GROUPS if sum(GROUPS) == pairs else (pairs,)
    half = n_left // 2
    side, local = left // half, lax.rem(left, half)
    near, far = side * half, (1 - side) * half
    across = [far + side * k + (1 - side) * (half - 1 - k) for k in range(half)]
    beside = [near + lax.rem(local + k, half) for k in range(1, half)]
    hops_right = sorted(range(1, n_right), key=lambda j: (abs(2 * j - n_right), j))

    table_copies = [
        pltpu.make_async_copy(src, dst, sem_t.at[i])
        for i, (src, dst) in enumerate((
            (hx_hbm, hx), (hy_hbm, hy), (wz_hbm, wz), (coup_hbm, coup_ref),
            (sx_hbm, sx_ref), (sy_hbm, sy_ref), (sz_hbm, sz_ref),
        ))
    ]

    def x_copy(pair):
        return pltpu.make_async_copy(
            x_hbm.at[:, pl.ds(2 * pair, 2)], x_buf.at[pair], sem_x.at[pair]
        )

    barrier = pltpu.get_barrier_semaphore()
    for other in across:
        pl.semaphore_signal(barrier, inc=1, device_id=(other, right), device_id_type=MESH)
    for k in range(1, half):
        @pl.when(local < k)
        def _():
            pl.semaphore_signal(
                barrier, inc=1, device_id=(near + k, right), device_id_type=MESH
            )
    for j in hops_right:
        pl.semaphore_signal(
            barrier, inc=1, device_id=(left, lax.rem(right + j, n_right)), device_id_type=MESH
        )
    table_copies[0].start()
    for pair in range(pairs):
        x_copy(pair).start()
    for copy in table_copies[1:]:
        copy.start()

    def left_copy(chunk, other, first_y=0, count_y=share_y):
        start, size = starts[chunk], sizes[chunk]
        return pltpu.make_async_remote_copy(
            src_ref=send_a.at[
                pl.ds(start * n_left + other * size, size), pl.ds(first_y, count_y)
            ],
            dst_ref=recv_b.at[left, pl.ds(start, size), pl.ds(first_y, count_y)],
            send_sem=sem_as.at[0],
            recv_sem=sem_br.at[chunk],
            device_id=(other, right),
            device_id_type=MESH,
        )

    def right_copy(chunk, j):
        other = lax.rem(right + j, n_right)
        rows = pl.ds(starts[chunk], sizes[chunk])
        return pltpu.make_async_remote_copy(
            src_ref=send_c.at[other, rows],
            dst_ref=recv_d.at[right, rows],
            send_sem=sem_cs.at[0],
            recv_sem=sem_dr.at[chunk],
            device_id=(left, other),
            device_id_type=MESH,
        )

    def wait_bytes(ref, sem):
        pltpu.make_async_copy(ref, ref, sem).wait()

    def left_arrived(chunk):
        rows = pl.ds(starts[chunk], sizes[chunk])
        wait_bytes(recv_b.at[pl.ds(0, n_left - 1), rows], sem_br.at[chunk])

    def right_arrived(chunk):
        rows = pl.ds(starts[chunk], sizes[chunk])
        wait_bytes(recv_d.at[pl.ds(0, n_right - 1), rows], sem_dr.at[chunk])

    flat_a = send_a.reshape(size_x * share_y, lanes)

    wide = WIDE if all(count % WIDE == 0 for count in groups) else 1

    def x_step(step, carry):
        planes = []
        for i in range(wide):
            x_copy(step * wide + i).wait()
            planes += [x_buf[step * wide + i, :, k].reshape(lanes, size_x) for k in range(2)]
        high, low = split(jnp.concatenate(planes, axis=0))
        dot = functools.partial(
            lax.dot_general,
            dimension_numbers=(((1,), (1,)), ((), ())),
            preferred_element_type=jnp.float32,
        )
        both = dot(hx[...], high)
        modes = both[:size_x] + both[size_x:] + dot(hx[:size_x], low)
        for i in range(2 * wide):
            flat_a[pl.ds(2 * wide * step + i, size_x, stride=share_y), :] = modes[
                :, i * lanes:(i + 1) * lanes
            ]
        return carry

    table_copies[0].wait()
    done = 0
    for count in groups:
        lax.fori_loop(done // wide, (done + count) // wide, x_step, 0)
        if done == 0:
            pl.semaphore_wait(barrier, half + local + n_right - 1)
        for other in across:
            left_copy(0, other, 2 * done, 2 * count).start()
        if done == 0:
            for k in range(half - 1):
                @pl.when(k < local)
                def _():
                    pl.semaphore_signal(
                        ready, inc=1, device_id=(near + k, right), device_id_type=MESH
                    )
        done += count

    @pl.when(local < half - 1)
    def _():
        pl.semaphore_wait(ready, half - 1 - local)

    for other in beside:
        left_copy(0, other).start()

    def left_advance(before, now):
        for chunk in range(1, len(sizes)):
            if before + WINDOW < ends[chunk] <= now + WINDOW:
                left_copy(chunk, across[0]).start()
            window = BACK if chunk >= len(sizes) - TAIL else WINDOW
            if before + window < ends[chunk] <= now + window:
                for other in across[1:] + beside:
                    left_copy(chunk, other).start()

    left_advance(-block_x, 0)

    for start, size in zip(starts, sizes):
        recv_b[left, pl.ds(start, size)] = send_a[pl.ds(start * n_left + left * size, size)]
    for copy in table_copies[1:]:
        copy.wait()
    sy_cols[...] = jnp.broadcast_to(sy_ref[...], (size_z, size_y)).T

    def y_stage(chunk):
        left_arrived(chunk)
        left_advance(starts[chunk], ends[chunk])
        start, size = starts[chunk], sizes[chunk]

        tall = TALL if size % TALL == 0 else 2

        def y_step(step, carry):
            first = start + tall * step
            rows = [recv_b[:, first + i].reshape(size_y, lanes) for i in range(tall)]
            high, low = split(jnp.concatenate(rows, axis=1))
            dot = functools.partial(jnp.dot, preferred_element_type=jnp.float32)
            both = dot(hy[...], high)
            modes = both[:size_y] + both[size_y:] + dot(hy[:size_y], low)
            for i in range(tall):
                send_c[:, first + i] = modes[:, i * lanes:(i + 1) * lanes].reshape(
                    n_right, block_y, lanes
                )
            return carry

        lax.fori_loop(0, size // tall, y_step, 0)
        for j in hops_right:
            right_copy(chunk, j).start()
        recv_d[right, pl.ds(start, size)] = send_c[right, pl.ds(start, size)]

    def z_stage(chunk):
        right_arrived(chunk)
        start, size = starts[chunk], sizes[chunk]
        count = size * block_y
        lines = [
            recv_d[r, pl.ds(start, size)].reshape(count, lanes) for r in range(n_right)
        ]
        high, low = split(jnp.concatenate(lines, axis=1))
        dot = functools.partial(jnp.dot, preferred_element_type=jnp.float32)
        both = dot(jnp.concatenate([high, low], axis=0), wz[0])
        z_buf[:count] = both[:count] + both[count:] + dot(high, wz[1])

        part_y = sy_cols[pl.ds(pl.multiple_of(right * block_y, block_y), block_y), :]

        def mix_step(step, carry):
            symbol = sx_ref[0, left * block_x + start + step] + part_y + sz_ref[...]
            weight = 1.0 / (1.0 + symbol)
            rest = 1.0 - weight
            rows = pl.ds(pl.multiple_of(step * block_y, block_y), block_y)
            old = [z_buf[rows, b * size_z:(b + 1) * size_z] for b in range(fields)]
            for a in range(fields):
                mixed = coup_ref[a, 0] * old[0]
                for b in range(1, fields):
                    mixed += coup_ref[a, b] * old[b]
                out_ref[a, start + step] = weight * old[a] + rest * mixed
            return carry

        lax.fori_loop(0, size, mix_step, 0)

    for chunk in range(len(sizes)):
        y_stage(chunk)
        if LAG <= chunk < len(sizes) - HOLD:
            z_stage(chunk - LAG)
    for chunk in range(max(len(sizes) - HOLD - LAG, 0), len(sizes)):
        z_stage(chunk)

    wait_bytes(send_a.at[pl.ds(0, (n_left - 1) * block_x)], sem_as.at[0])
    wait_bytes(send_c.at[pl.ds(0, n_right - 1)], sem_cs.at[0])


def solution(mesh):
    n_left, n_right = mesh.shape["left"], mesh.shape["right"]

    def body(species, coupling, symbol_x, symbol_y, symbol_z):
        fields, size_x, share_y, share_z = species.shape
        size_y, size_z = symbol_y.shape[0], symbol_z.shape[0]
        lanes = fields * share_z
        block_x, block_y = size_x // n_left, size_y // n_right
        sizes = chunk_sizes(block_x)
        chunks = len(sizes)

        order = np.concatenate([
            np.arange(size_x).reshape(n_left, block_x)[:, sum(sizes[:c]):sum(sizes[:c + 1])].ravel()
            for c in range(chunks)
        ])
        hx = np.concatenate(halves(basis_table(size_x)[order]))
        hy = np.concatenate(halves(basis_table(size_y)))
        hz = basis_table(size_z).reshape(n_right, share_z, size_z)
        wz = np.einsum("rzn,fg->rfzgn", hz, np.eye(fields))
        wz = np.stack(halves(wz.reshape(n_right * lanes, fields * size_z)))

        hbm = pl.BlockSpec(memory_space=pltpu.HBM)
        vmem = pl.BlockSpec(memory_space=pltpu.VMEM)
        f32, bf16 = jnp.float32, jnp.bfloat16
        room = 64 * 2 ** 20 - 2 * (4 * fields * block_x * block_y * size_z)
        return pl.pallas_call(
            functools.partial(kernel, n_left, n_right, sizes),
            out_shape=pltpu.VMEM((fields, block_x, block_y, size_z), f32),
            in_specs=[hbm] * 8,
            out_specs=vmem,
            scratch_shapes=[
                pltpu.VMEM((share_y // 2, fields, 2, share_z, size_x), f32),
                pltpu.VMEM(hx.shape, bf16),
                pltpu.VMEM(hy.shape, bf16),
                pltpu.VMEM(wz.shape, bf16),
                pltpu.SMEM(coupling.shape, f32),
                pltpu.SMEM((1, size_x), f32),
                pltpu.VMEM((1, size_y), f32),
                pltpu.VMEM((1, size_z), f32),
                pltpu.VMEM((size_x, share_y, lanes), f32),
                pltpu.VMEM((n_left, block_x, share_y, lanes), f32),
                pltpu.VMEM((n_right, block_x, block_y, lanes), f32),
                pltpu.VMEM((n_right, block_x, block_y, lanes), f32),
                pltpu.VMEM((max(sizes) * block_y, fields * size_z), f32),
                pltpu.VMEM((size_y, size_z), f32),
                pltpu.SemaphoreType.DMA((share_y // 2,)),
                pltpu.SemaphoreType.DMA((7,)),
                pltpu.SemaphoreType.DMA((1,)),
                pltpu.SemaphoreType.DMA((chunks,)),
                pltpu.SemaphoreType.DMA((1,)),
                pltpu.SemaphoreType.DMA((chunks,)),
                pltpu.SemaphoreType.REGULAR,
            ],
            compiler_params=pltpu.CompilerParams(
                collective_id=0, has_side_effects=True, vmem_limit_bytes=room
            ),
        )(
            jnp.transpose(species, (0, 2, 3, 1)), jnp.asarray(hx), jnp.asarray(hy),
            jnp.asarray(wz), coupling, symbol_x[None], symbol_y[None], symbol_z[None],
        )

    in_specs = (P(None, None, "left", "right"), P(), P(), P(), P())
    out_specs = P(None, "left", "right", None)
    return jax.shard_map(body, mesh=mesh, in_specs=in_specs, out_specs=out_specs, check_vma=False)
```

```python
import functools

import jax
import jax.numpy as jnp
import numpy as np
from jax import lax
from jax.experimental import pallas as pl
from jax.experimental.pallas import tpu as pltpu
from jax.sharding import PartitionSpec as P

MESH = pl.DeviceIdType.MESH
PARTS = (4, 4, 4, 4, 4, 4, 2, 2, 2, 2)
GROUPS = (2, 2, 4)
WINDOW = 12
TAIL = 2
BACK = 4
WIDE = 2
TALL = 4
LAG = 2
HOLD = 3


def chunk_sizes(block):
    unit = block // sum(PARTS)
    return [part * unit for part in PARTS] if unit and block % sum(PARTS) == 0 else [block]


def basis_table(count):
    rank = np.arange(count)
    angle = 2.0 * np.pi / count * (rank[:, None] * rank[None, :] % count)
    return (np.cos(angle) + np.sin(angle)) / np.sqrt(count)


def halves(table):
    table = table.astype(np.float32)
    high = table.astype(jnp.bfloat16)
    low = (table - high.astype(np.float32)).astype(jnp.bfloat16)
    return high, low


def split(values):
    high = values.astype(jnp.bfloat16)
    low = (values - high.astype(jnp.float32)).astype(jnp.bfloat16)
    return high, low


def kernel(
    n_left, n_right, sizes,
    x_hbm, hx_hbm, hy_hbm, wz_hbm, coup_hbm, sx_hbm, sy_hbm, sz_hbm,
    out_ref,
    x_buf, hx, hy, wz, coup_ref, sx_ref, sy_ref, sz_ref, send_a, recv_b, send_c, recv_d, z_buf, sy_cols,
    sem_x, sem_t, sem_as, sem_br, sem_cs, sem_dr, ready,
):
    fields, share_y, share_z, size_x = x_hbm.shape
    size_y, size_z = sy_hbm.shape[1], sz_hbm.shape[1]
    lanes = fields * share_z
    block_x, block_y = size_x // n_left, size_y // n_right
    pairs = share_y // 2
    starts = [sum(sizes[:c]) for c in range(len(sizes))]
    left, right = lax.axis_index("left"), lax.axis_index("right")
    ends = [start + size for start, size in zip(starts, sizes)]
    groups = GROUPS if sum(GROUPS) == pairs else (pairs,)
    half = n_left // 2
    side, local = left // half, lax.rem(left, half)
    near, far = side * half, (1 - side) * half
    across = [far + side * k + (1 - side) * (half - 1 - k) for k in range(half)]
    beside = [near + lax.rem(local + k, half) for k in range(1, half)]
    hops_right = sorted(range(1, n_right), key=lambda j: (abs(2 * j - n_right), j))

    table_copies = [
        pltpu.make_async_copy(src, dst, sem_t.at[i])
        for i, (src, dst) in enumerate((
            (hx_hbm, hx), (hy_hbm, hy), (wz_hbm, wz), (coup_hbm, coup_ref),
            (sx_hbm, sx_ref), (sy_hbm, sy_ref), (sz_hbm, sz_ref),
        ))
    ]

    def x_copy(pair):
        return pltpu.make_async_copy(
            x_hbm.at[:, pl.ds(2 * pair, 2)], x_buf.at[pair], sem_x.at[pair]
        )

    barrier = pltpu.get_barrier_semaphore()
    for other in across:
        pl.semaphore_signal(barrier, inc=1, device_id=(other, right), device_id_type=MESH)
    for k in range(1, half):
        @pl.when(local < k)
        def _():
            pl.semaphore_signal(
                barrier, inc=1, device_id=(near + k, right), device_id_type=MESH
            )
    for j in hops_right:
        pl.semaphore_signal(
            barrier, inc=1, device_id=(left, lax.rem(right + j, n_right)), device_id_type=MESH
        )
    table_copies[0].start()
    for pair in range(pairs):
        x_copy(pair).start()
    for copy in table_copies[1:]:
        copy.start()

    def left_copy(chunk, other, first_y=0, count_y=share_y):
        start, size = starts[chunk], sizes[chunk]
        return pltpu.make_async_remote_copy(
            src_ref=send_a.at[
                pl.ds(start * n_left + other * size, size), pl.ds(first_y, count_y)
            ],
            dst_ref=recv_b.at[left, pl.ds(start, size), pl.ds(first_y, count_y)],
            send_sem=sem_as.at[0],
            recv_sem=sem_br.at[chunk],
            device_id=(other, right),
            device_id_type=MESH,
        )

    def right_copy(chunk, j):
        other = lax.rem(right + j, n_right)
        rows = pl.ds(starts[chunk], sizes[chunk])
        return pltpu.make_async_remote_copy(
            src_ref=send_c.at[other, rows],
            dst_ref=recv_d.at[right, rows],
            send_sem=sem_cs.at[0],
            recv_sem=sem_dr.at[chunk],
            device_id=(left, other),
            device_id_type=MESH,
        )

    def wait_bytes(ref, sem):
        pltpu.make_async_copy(ref, ref, sem).wait()

    def left_arrived(chunk):
        rows = pl.ds(starts[chunk], sizes[chunk])
        wait_bytes(recv_b.at[pl.ds(0, n_left - 1), rows], sem_br.at[chunk])

    def right_arrived(chunk):
        rows = pl.ds(starts[chunk], sizes[chunk])
        wait_bytes(recv_d.at[pl.ds(0, n_right - 1), rows], sem_dr.at[chunk])

    flat_a = send_a.reshape(size_x * share_y, lanes)

    wide = WIDE if all(count % WIDE == 0 for count in groups) else 1

    def x_step(step, carry):
        planes = []
        for i in range(wide):
            x_copy(step * wide + i).wait()
            planes += [x_buf[step * wide + i, :, k].reshape(lanes, size_x) for k in range(2)]
        high, low = split(jnp.concatenate(planes, axis=0))
        dot = functools.partial(
            lax.dot_general,
            dimension_numbers=(((1,), (1,)), ((), ())),
            preferred_element_type=jnp.float32,
        )
        both = dot(hx[...], high)
        modes = both[:size_x] + both[size_x:] + dot(hx[:size_x], low)
        for i in range(2 * wide):
            flat_a[pl.ds(2 * wide * step + i, size_x, stride=share_y), :] = modes[
                :, i * lanes:(i + 1) * lanes
            ]
        return carry

    table_copies[0].wait()
    done = 0
    for count in groups:
        lax.fori_loop(done // wide, (done + count) // wide, x_step, 0)
        if done == 0:
            pl.semaphore_wait(barrier, half + local + n_right - 1)
        for other in across:
            left_copy(0, other, 2 * done, 2 * count).start()
        if done == 0:
            for k in range(half - 1):
                @pl.when(k < local)
                def _():
                    pl.semaphore_signal(
                        ready, inc=1, device_id=(near + k, right), device_id_type=MESH
                    )
        done += count

    @pl.when(local < half - 1)
    def _():
        pl.semaphore_wait(ready, half - 1 - local)

    for other in beside:
        left_copy(0, other).start()

    def left_advance(before, now):
        for chunk in range(1, len(sizes)):
            if before + WINDOW < ends[chunk] <= now + WINDOW:
                left_copy(chunk, across[0]).start()
            window = BACK if chunk >= len(sizes) - TAIL else WINDOW
            if before + window < ends[chunk] <= now + window:
                for other in across[1:] + beside:
                    left_copy(chunk, other).start()

    left_advance(-block_x, 0)

    for start, size in zip(starts, sizes):
        recv_b[left, pl.ds(start, size)] = send_a[pl.ds(start * n_left + left * size, size)]
    for copy in table_copies[1:]:
        copy.wait()
    sy_cols[...] = jnp.broadcast_to(sy_ref[...], (size_z, size_y)).T

    def y_stage(chunk):
        left_arrived(chunk)
        left_advance(starts[chunk], ends[chunk])
        start, size = starts[chunk], sizes[chunk]

        tall = TALL if size % TALL == 0 else 2

        def y_step(step, carry):
            first = start + tall * step
            rows = [recv_b[:, first + i].reshape(size_y, lanes) for i in range(tall)]
            high, low = split(jnp.concatenate(rows, axis=1))
            dot = functools.partial(jnp.dot, preferred_element_type=jnp.float32)
            both = dot(hy[...], high)
            modes = both[:size_y] + both[size_y:] + dot(hy[:size_y], low)
            for i in range(tall):
                send_c[:, first + i] = modes[:, i * lanes:(i + 1) * lanes].reshape(
                    n_right, block_y, lanes
                )
            return carry

        lax.fori_loop(0, size // tall, y_step, 0)
        for j in hops_right:
            right_copy(chunk, j).start()
        recv_d[right, pl.ds(start, size)] = send_c[right, pl.ds(start, size)]

    def z_stage(chunk):
        right_arrived(chunk)
        start, size = starts[chunk], sizes[chunk]
        count = size * block_y
        lines = [
            recv_d[r, pl.ds(start, size)].reshape(count, lanes) for r in range(n_right)
        ]
        high, low = split(jnp.concatenate(lines, axis=1))
        dot = functools.partial(jnp.dot, preferred_element_type=jnp.float32)
        both = dot(jnp.concatenate([high, low], axis=0), wz[0])
        z_buf[:count] = both[:count] + both[count:] + dot(high, wz[1])

        part_y = sy_cols[pl.ds(pl.multiple_of(right * block_y, block_y), block_y), :]

        def mix_step(step, carry):
            symbol = sx_ref[0, left * block_x + start + step] + part_y + sz_ref[...]
            weight = 1.0 / (1.0 + symbol)
            rest = 1.0 - weight
            rows = pl.ds(pl.multiple_of(step * block_y, block_y), block_y)
            old = [z_buf[rows, b * size_z:(b + 1) * size_z] for b in range(fields)]
            for a in range(fields):
                mixed = coup_ref[a, 0] * old[0]
                for b in range(1, fields):
                    mixed += coup_ref[a, b] * old[b]
                out_ref[a, start + step] = weight * old[a] + rest * mixed
            return carry

        lax.fori_loop(0, size, mix_step, 0)

    for chunk in range(len(sizes)):
        y_stage(chunk)
        if LAG <= chunk < len(sizes) - HOLD:
            z_stage(chunk - LAG)
    for chunk in range(max(len(sizes) - HOLD - LAG, 0), len(sizes)):
        z_stage(chunk)

    wait_bytes(send_a.at[pl.ds(0, (n_left - 1) * block_x)], sem_as.at[0])
    wait_bytes(send_c.at[pl.ds(0, n_right - 1)], sem_cs.at[0])


def solution(mesh):
    n_left, n_right = mesh.shape["left"], mesh.shape["right"]

    def body(species, coupling, symbol_x, symbol_y, symbol_z):
        fields, size_x, share_y, share_z = species.shape
        size_y, size_z = symbol_y.shape[0], symbol_z.shape[0]
        lanes = fields * share_z
        block_x, block_y = size_x // n_left, size_y // n_right
        sizes = chunk_sizes(block_x)
        chunks = len(sizes)

        order = np.concatenate([
            np.arange(size_x).reshape(n_left, block_x)[:, sum(sizes[:c]):sum(sizes[:c + 1])].ravel()
            for c in range(chunks)
        ])
        hx = np.concatenate(halves(basis_table(size_x)[order]))
        hy = np.concatenate(halves(basis_table(size_y)))
        hz = basis_table(size_z).reshape(n_right, share_z, size_z)
        wz = np.einsum("rzn,fg->rfzgn", hz, np.eye(fields))
        wz = np.stack(halves(wz.reshape(n_right * lanes, fields * size_z)))

        hbm = pl.BlockSpec(memory_space=pltpu.HBM)
        vmem = pl.BlockSpec(memory_space=pltpu.VMEM)
        f32, bf16 = jnp.float32, jnp.bfloat16
        room = 64 * 2 ** 20 - 2 * (4 * fields * block_x * block_y * size_z)
        return pl.pallas_call(
            functools.partial(kernel, n_left, n_right, sizes),
            out_shape=pltpu.VMEM((fields, block_x, block_y, size_z), f32),
            in_specs=[hbm] * 8,
            out_specs=vmem,
            scratch_shapes=[
                pltpu.VMEM((share_y // 2, fields, 2, share_z, size_x), f32),
                pltpu.VMEM(hx.shape, bf16),
                pltpu.VMEM(hy.shape, bf16),
                pltpu.VMEM(wz.shape, bf16),
                pltpu.SMEM(coupling.shape, f32),
                pltpu.SMEM((1, size_x), f32),
                pltpu.VMEM((1, size_y), f32),
                pltpu.VMEM((1, size_z), f32),
                pltpu.VMEM((size_x, share_y, lanes), f32),
                pltpu.VMEM((n_left, block_x, share_y, lanes), f32),
                pltpu.VMEM((n_right, block_x, block_y, lanes), f32),
                pltpu.VMEM((n_right, block_x, block_y, lanes), f32),
                pltpu.VMEM((max(sizes) * block_y, fields * size_z), f32),
                pltpu.VMEM((size_y, size_z), f32),
                pltpu.SemaphoreType.DMA((share_y // 2,)),
                pltpu.SemaphoreType.DMA((7,)),
                pltpu.SemaphoreType.DMA((1,)),
                pltpu.SemaphoreType.DMA((chunks,)),
                pltpu.SemaphoreType.DMA((1,)),
                pltpu.SemaphoreType.DMA((chunks,)),
                pltpu.SemaphoreType.REGULAR,
            ],
            compiler_params=pltpu.CompilerParams(
                collective_id=0, has_side_effects=True, vmem_limit_bytes=room
            ),
        )(
            jnp.transpose(species, (0, 2, 3, 1)), jnp.asarray(hx), jnp.asarray(hy),
            jnp.asarray(wz), coupling, symbol_x[None], symbol_y[None], symbol_z[None],
        )

    in_specs = (P(None, None, "left", "right"), P(), P(), P(), P())
    out_specs = P(None, "left", "right", None)
    return jax.shard_map(body, mesh=mesh, in_specs=in_specs, out_specs=out_specs, check_vma=False)
```
